16 devices in a mesh: proto: 4 (over z, y), data: 4 (over x, core).
Axes of the slice: x: 2, y: 2, z: 2, core: 2. Of those that a mesh axis runs over, the one named last changes fastest.
Arguments:
- emb_one: bfloat16 [8192, 256], P('data')
- emb_two: bfloat16 [8192, 256], P('data')
- protos: bfloat16 [1024, 256], P('proto')
Outputs:
- output 1: float32 [8192, 1024], P('data', 'proto')
- output 2: float32 [8192, 1024], P('data', 'proto')
- output 3: float32 [], replicated
- output 4: float32 [8192, 256], P('data')
- output 5: float32 [8192, 256], P('data')
- output 6: float32 [1024, 256], P('proto')
All inputs are finite; a program needn't handle non-finite values.
Results may differ from the reference program's by a relative error of at most 0.001.
Values are sent between devices in bfloat16 or wider.
A program may use at most 1 GiB of HBM per device.

```python
import jax
import jax.numpy as jnp

ROWS_DEV = 2048
DATA_GROUPS = 4
NUM_PROTOS = 1024
EMBED_DIM = 256
SINKHORN_ITERS = 3
EPSILON = 0.05
TEMP_TAU = 0.1
NOISE_SCALE = 0.8
TOTAL_ROWS = ROWS_DEV * DATA_GROUPS


def unit_rows(matrix):
    return matrix / jnp.sqrt(jnp.sum(matrix * matrix, axis=1, keepdims=True))


def setup_inputs(seed: int = 0) -> dict:
    key = jax.random.key(seed)
    key_protos, key_home, key_one, key_two = jax.random.split(key, 4)
    protos = unit_rows(jax.random.normal(key_protos, (NUM_PROTOS, EMBED_DIM), jnp.float32))
    shard_ids = jnp.arange(TOTAL_ROWS, dtype=jnp.int32) // ROWS_DEV
    home_ids = shard_ids + DATA_GROUPS * jax.random.randint(key_home, (TOTAL_ROWS,), 0, NUM_PROTOS // DATA_GROUPS)
    centers = protos[home_ids]
    noise_one = jax.random.normal(key_one, (TOTAL_ROWS, EMBED_DIM), jnp.float32) * (NOISE_SCALE * EMBED_DIM ** -0.5)
    noise_two = jax.random.normal(key_two, (TOTAL_ROWS, EMBED_DIM), jnp.float32) * (NOISE_SCALE * EMBED_DIM ** -0.5)
    return {'emb_one': unit_rows(centers + noise_one).astype(jnp.bfloat16),
            'emb_two': unit_rows(centers + noise_two).astype(jnp.bfloat16),
            'protos': protos.astype(jnp.bfloat16)}


def sinkhorn_codes(scores):
    transport = jnp.exp(scores / EPSILON)
    for _ in range(SINKHORN_ITERS):
        col_sum = jnp.sum(transport, axis=0)
        transport = transport / (NUM_PROTOS * col_sum)
        row_sum = jnp.sum(transport, axis=1, keepdims=True)
        transport = transport / (TOTAL_ROWS * row_sum)
    return TOTAL_ROWS * transport


def log_probs(scores):
    logits = scores / TEMP_TAU
    return logits - jnp.log(jnp.sum(jnp.exp(logits), axis=1, keepdims=True))


def reference(emb_one, emb_two, protos):
    scores_one = jnp.dot(emb_one, protos.T, preferred_element_type=jnp.float32)
    scores_two = jnp.dot(emb_two, protos.T, preferred_element_type=jnp.float32)
    codes_one = sinkhorn_codes(scores_one)
    codes_two = sinkhorn_codes(scores_two)
    logp_one = log_probs(scores_one)
    logp_two = log_probs(scores_two)
    loss_value = -(jnp.sum(codes_two * logp_one) + jnp.sum(codes_one * logp_two)) / (2 * TOTAL_ROWS)
    grad_scale = 2 * TOTAL_ROWS * TEMP_TAU
    logit_grad_one = ((jnp.exp(logp_one) - codes_two) / grad_scale).astype(jnp.bfloat16)
    logit_grad_two = ((jnp.exp(logp_two) - codes_one) / grad_scale).astype(jnp.bfloat16)
    grad_one = jnp.dot(logit_grad_one, protos, preferred_element_type=jnp.float32)
    grad_two = jnp.dot(logit_grad_two, protos, preferred_element_type=jnp.float32)
    grad_protos = (jnp.dot(logit_grad_one.T, emb_one, preferred_element_type=jnp.float32)
                   + jnp.dot(logit_grad_two.T, emb_two, preferred_element_type=jnp.float32))
    return codes_one, codes_two, loss_value, grad_one, grad_two, grad_protos
```

```python
import functools
import math

import jax
import jax.numpy as jnp
from jax import lax
from jax.experimental import pallas as pl
from jax.experimental.pallas import tpu as pltpu
from jax.sharding import PartitionSpec as P

EPSILON = 0.05
TEMP_TAU = 0.1
ITERS = 3
MESH = pl.DeviceIdType.MESH
F32 = jnp.float32
LOG2E = math.log2(math.e)


def lanes(x):
    total = x[:, :128]
    for i in range(1, x.shape[1] // 128):
        total = total + x[:, i * 128:(i + 1) * 128]
    return total


def subl(x):
    return jnp.sum(x.reshape(x.shape[0] // 8, 8, x.shape[1]), axis=0)


def kernel(np_, nd, z1_ref, z2_ref, c_ref,
           code1, code2, loss_ref, g1, g2, gc,
           z, call, e, c1b, cb, dinv, h, hown, vb, dcp, dcr, dcs, lossb,
           lsem, csend, crecv, c1send, c1recv, bsend, brecv, dsend, drecv, lsend, lrecv):
    rows, kb = z.shape[1], call.shape[1]
    nrows, nk = rows * nd, kb * np_
    p, d = lax.axis_index("proto"), lax.axis_index("data")
    codes, grads = (code1, code2), (g1, g2)

    def remote(src, dst, ss, rs, pp, dd):
        return pltpu.make_async_remote_copy(src_ref=src, dst_ref=dst, send_sem=ss, recv_sem=rs,
                                            device_id={"proto": pp, "data": dd}, device_id_type=MESH)

    loads = [pltpu.make_async_copy(c_ref, call.at[p], lsem.at[0]),
             pltpu.make_async_copy(z1_ref, z.at[0], lsem.at[1]),
             pltpu.make_async_copy(z2_ref, z.at[1], lsem.at[2])]
    for cp in loads:
        cp.start()
    others = [(i, j) for i in range(np_) for j in range(nd) if i or j]
    barrier = pltpu.get_barrier_semaphore()
    for i, j in others:
        pl.semaphore_signal(barrier, inc=1, device_id={"proto": (p + i) % np_, "data": (d + j) % nd},
                            device_id_type=MESH)
    loads[0].wait()
    pl.semaphore_wait(barrier, len(others))

    gathers = []
    for q in range(1, np_):
        cp = remote(call.at[p], call.at[p], csend.at[q], crecv.at[q], (p + q) % np_, d)
        cp.start()
        gathers.append(cp)

    def scores(v, b, r):
        return lax.dot_general(z[v, r, :], call[b], (((1,), (1,)), ((), ())), preferred_element_type=F32)

    def chunk(i, size):
        return pl.ds(pl.multiple_of(i * size, size), size)

    RC = 256

    def exp_block(v, b, total):
        def body(i, acc):
            r = chunk(i, RC)
            x = jnp.exp2(scores(v, b, r) * (LOG2E / TEMP_TAU))
            e[v, b, r, :] = x
            return acc + subl(x * x) if total else acc
        return lax.fori_loop(0, rows // RC, body, jnp.zeros((8, kb), F32))

    own = []
    for v in range(2):
        loads[1 + v].wait()
        own.append(jnp.sum(exp_block(v, p, True), axis=0, keepdims=True))
    c1b[d * np_ + p] = jnp.concatenate(own, axis=0)
    firsts = []
    for n, (i, j) in enumerate(others):
        me = c1b.at[d * np_ + p]
        cp = remote(me, me, c1send.at[n], c1recv.at[n], (p + i) % np_, (d + j) % nd)
        cp.start()
        firsts.append(cp)

    for q in range(1, np_):
        gathers[q - 1].wait_recv()
        b = (p + np_ - q) % np_
        for v in range(2):
            exp_block(v, b, False)
    for cp in firsts:
        cp.wait_recv()
    for v in range(2):
        for b in range(np_):
            tot = c1b[b, v:v + 1, :]
            for j in range(1, nd):
                tot = tot + c1b[j * np_ + b, v:v + 1, :]
            vb[v, b] = jnp.broadcast_to(1.0 / (nk * tot), (8, kb))

    R2 = 64

    def scaled(v, b, r):
        x = e[v, b, r, :]
        n = r.size // 8
        return x, ((x * x).reshape(n, 8, kb) * vb[v, b][None]).reshape(n * 8, kb)

    def sweep(v, first):
        def body(i, accs):
            r = chunk(i, R2)
            racc = dacc = None
            for b in range(np_):
                x, t = scaled(v, b, r)
                t = lanes(t)
                racc = t if racc is None else racc + t
                if first:
                    s = lanes(x)
                    dacc = s if dacc is None else dacc + s
            u = 1.0 / (nrows * jnp.sum(racc, axis=1, keepdims=True))
            if first:
                dinv[v, r, :] = jnp.broadcast_to(jnp.sum(dacc, axis=1, keepdims=True), (R2, 128))
            out = []
            for b in range(np_):
                x = e[v, b, r, :]
                out.append(accs[b] + subl(x * x * u))
            return tuple(out)
        return lax.fori_loop(0, rows // R2, body, tuple(jnp.zeros((8, kb), F32) for _ in range(np_)))

    def exchange(it, v, accs):
        slot = (it * 2 + v) * nd
        for b in range(np_):
            cb[slot + d, :, b * kb:(b + 1) * kb] = jnp.sum(accs[b], axis=0, keepdims=True)
        out = []
        for q in range(1, nd):
            me = cb.at[slot + d]
            cp = remote(me, me, bsend.at[slot + q], brecv.at[slot + q], p, (d + q) % nd)
            cp.start()
            out.append(cp)
        return out

    def finish(it, v, copies):
        slot = (it * 2 + v) * nd
        for cp in copies:
            cp.wait_recv()
        tot = cb[slot]
        for j in range(1, nd):
            tot = tot + cb[slot + j]
        inv = 1.0 / (nk * tot)
        for b in range(np_):
            vb[v, b] = jnp.broadcast_to(inv[:, b * kb:(b + 1) * kb], (8, kb))

    pend, sends = [None, None], []
    for it in range(ITERS - 1):
        for v in range(2):
            if it:
                finish(it - 1, v, pend[v])
            pend[v] = exchange(it, v, sweep(v, it == 0))
            sends += pend[v]
    for v in range(2):
        finish(ITERS - 2, v, pend[v])

    R3 = 128
    scale = 1.0 / (2 * nrows * TEMP_TAU)

    def last(i, lacc):
        r = chunk(i, R3)
        rinv = []
        for v in range(2):
            racc = None
            for b in range(np_):
                t = lanes(scaled(v, b, r)[1])
                racc = t if racc is None else racc + t
            rinv.append(1.0 / jnp.sum(racc, axis=1, keepdims=True))
        den = [dinv[v, r, :] for v in range(2)]
        for v in range(2):
            w = 1 - v
            di = (scale / den[w])
            di = jnp.concatenate([di, di], axis=1)
            rs = rinv[v] * scale
            for b in range(np_):
                q = scaled(v, b, r)[1] * rs
                h[w, :, b * kb:(b + 1) * kb] = (e[w, b, r, :] * di - q).astype(jnp.bfloat16)
        for v in range(2):
            acc = None
            for b in range(np_):
                x = jnp.dot(h[v, :, b * kb:(b + 1) * kb], call[b], preferred_element_type=F32)
                acc = x if acc is None else acc + x
            grads[v][r, :] = acc
        for v in range(2):
            w = 1 - v
            x, t = scaled(v, p, r)
            q = t * rinv[v]
            codes[v][r, :] = q
            di = scale / den[w]
            di = jnp.concatenate([di, di], axis=1)
            hown[w, r, :] = (e[w, p, r, :] * di - t * (rinv[v] * scale)).astype(jnp.bfloat16)
            ld = jnp.log(den[w])
            logp = scores(w, p, r) * (1.0 / TEMP_TAU) - jnp.concatenate([ld, ld], axis=1)
            lacc = lacc + subl(lanes(q * logp))
        return lacc

    lacc = lax.fori_loop(0, rows // R3, last, jnp.zeros((8, 128), F32))
    dims = (((0,), (0,)), ((), ()))
    dcp[...] = (lax.dot_general(hown[0], z[0], dims, preferred_element_type=F32)
                + lax.dot_general(hown[1], z[1], dims, preferred_element_type=F32)).reshape(dcp.shape)
    core = d % 2
    mate, across = d + 1 - 2 * core, (d + 2) % nd
    s1 = remote(dcp.at[1 - core], dcr.at[0], dsend.at[0], drecv.at[0], p, mate)
    s1.start()
    lossb[d * np_ + p] = jnp.broadcast_to(jnp.sum(lacc).reshape(1, 1), (1, 128))
    lcopies = []
    for n, (i, j) in enumerate(others):
        me = lossb.at[d * np_ + p]
        cp = remote(me, me, lsend.at[n], lrecv.at[n], (p + i) % np_, (d + j) % nd)
        cp.start()
        lcopies.append(cp)
    s1.wait_recv()
    dcs[...] = dcp[core] + dcr[0]
    s2 = remote(dcs, dcr.at[1], dsend.at[1], drecv.at[1], p, across)
    s2.start()
    for cp in lcopies:
        cp.wait_recv()
    tot = lossb[0]
    for n in range(1, np_ * nd):
        tot = tot + lossb[n]
    loss_ref[0, 0] = jnp.sum(tot[:, :1]) * (-1.0 / (2 * nrows))
    s2.wait_recv()
    half = kb // 2
    mine = gc.at[pl.ds(pl.multiple_of(core * half, half), half), :]
    mine[...] = dcs[...] + dcr[1]
    s3 = remote(mine, mine, dsend.at[2], drecv.at[2], p, mate)
    s3.start()
    s3.wait_recv()
    for cp in gathers + firsts + sends + [s1, s2, s3] + lcopies:
        cp.wait_send()


def solution(mesh):
    np_, nd = mesh.shape["proto"], mesh.shape["data"]

    def step(emb_one, emb_two, protos):
        rows, dim = emb_one.shape
        kb = protos.shape[0]
        n, dma = np_ * nd, pltpu.SemaphoreType.DMA
        nx = (ITERS - 1) * 2 * nd
        vm, anym = pl.BlockSpec(memory_space=pltpu.VMEM), pl.BlockSpec(memory_space=pl.ANY)
        sds = jax.ShapeDtypeStruct
        out = pl.pallas_call(
            functools.partial(kernel, np_, nd),
            out_shape=(sds((rows, kb), F32), sds((rows, kb), F32), sds((1, 1), F32),
                       sds((rows, dim), F32), sds((rows, dim), F32), sds((kb, dim), F32)),
            in_specs=[anym] * 3,
            out_specs=(vm, vm, pl.BlockSpec(memory_space=pltpu.SMEM), vm, vm, vm),
            scratch_shapes=[
                pltpu.VMEM((2, rows, dim), jnp.bfloat16),
                pltpu.VMEM((np_, kb, dim), jnp.bfloat16),
                pltpu.VMEM((2, np_, rows, kb), F32),
                pltpu.VMEM((n, 2, kb), F32),
                pltpu.VMEM((nx, 1, np_ * kb), F32),
                pltpu.VMEM((2, rows, 128), F32),
                pltpu.VMEM((2, 128, np_ * kb), jnp.bfloat16),
                pltpu.VMEM((2, rows, kb), jnp.bfloat16),
                pltpu.VMEM((2, np_, 8, kb), F32),
                pltpu.VMEM((2, kb // 2, dim), F32),
                pltpu.VMEM((2, kb // 2, dim), F32),
                pltpu.VMEM((kb // 2, dim), F32),
                pltpu.VMEM((n, 1, 128), F32),
                dma((3,)), dma((np_,)), dma((np_,)), dma((n - 1,)), dma((n - 1,)),
                dma((nx,)), dma((nx,)), dma((3,)), dma((3,)), dma((n - 1,)), dma((n - 1,)),
            ],
            compiler_params=pltpu.CompilerParams(collective_id=0, has_side_effects=True,
                                                 vmem_limit_bytes=48 * 1024 * 1024),
        )(emb_one, emb_two, protos)
        code1, code2, loss, g1, g2, gc = out
        return code1, code2, loss.reshape(()), g1, g2, gc

    return jax.shard_map(
        step, mesh=mesh,
        in_specs=(P("data", None), P("data", None), P("proto", None)),
        out_specs=(P("data", "proto"), P("data", "proto"), P(), P("data", None), P("data", None), P("proto", None)),
        check_vma=False)
```

```python
import functools
import math

import jax
import jax.numpy as jnp
from jax import lax
from jax.experimental import pallas as pl
from jax.experimental.pallas import tpu as pltpu
from jax.sharding import PartitionSpec as P

EPSILON = 0.05
TEMP_TAU = 0.1
ITERS = 3
VMEM_MIB = 48
MESH = pl.DeviceIdType.MESH
F32 = jnp.float32
LOG2E = math.log2(math.e)


def lanes(x):
    total = x[:, :128]
    for i in range(1, x.shape[1] // 128):
        total = total + x[:, i * 128:(i + 1) * 128]
    return total


def subl(x):
    return jnp.sum(x.reshape(x.shape[0] // 8, 8, x.shape[1]), axis=0)


def kernel(np_, nd, z1_ref, z2_ref, c_ref,
           code1, code2, loss_ref, g1, g2, gc,
           z, call, e, a2, c1b, cb, dsum, di, rs, hown, vb, dcp, dcr, dcs, lossb,
           lsem, csend, crecv, fsend, frecv, c1send, c1recv, bsend, brecv, dsend, drecv, lsend, lrecv):
    rows, kb = z.shape[1], 2 * call.shape[2]
    nrows, nk = rows * nd, kb * np_
    p, d = lax.axis_index("proto"), lax.axis_index("data")
    core = d % 2
    mate, across = d + 1 - 2 * core, (d + 2) % nd
    codes, grads = (code1, code2), (g1, g2)
    near = p + 1 - 2 * (p % 2)
    peers = (near, (p + 2) % np_, (near + 2) % np_)

    def remote(src, dst, ss, rsem, pp, dd):
        return pltpu.make_async_remote_copy(src_ref=src, dst_ref=dst, send_sem=ss, recv_sem=rsem,
                                            device_id={"proto": pp, "data": dd}, device_id_type=MESH)

    half = kb // 2
    loads = [pltpu.make_async_copy(c_ref.at[pl.ds(0, half), :], call.at[p, 0], lsem.at[0]),
             pltpu.make_async_copy(c_ref.at[pl.ds(half, half), :], call.at[p, 1], lsem.at[1]),
             pltpu.make_async_copy(z1_ref, z.at[0], lsem.at[2]),
             pltpu.make_async_copy(z2_ref, z.at[1], lsem.at[3])]
    for cp in loads:
        cp.start()
    others = [(i, j) for i in range(np_) for j in range(nd) if i or j]
    barrier = pltpu.get_barrier_semaphore()
    for i, j in others:
        pl.semaphore_signal(barrier, inc=1, device_id={"proto": (p + i) % np_, "data": (d + j) % nd},
                            device_id_type=MESH)
    loads[0].wait()
    loads[1].wait()
    pl.semaphore_wait(barrier, len(others))

    gathers = []
    for n, peer in enumerate(peers):
        cp = remote(call.at[p, core], call.at[p, core], csend.at[n], crecv.at[n], peer, d)
        cp.start()
        gathers.append(cp)

    def scores(v, b, r):
        return lax.dot_general(z[v, r, :], call[b].reshape(kb, call.shape[3]), (((1,), (1,)), ((), ())),
                               preferred_element_type=F32)

    def chunk(i, size):
        return pl.ds(pl.multiple_of(i * size, size), size)

    RC = 512

    def exp_block(v, b, n):
        def body(i, acc):
            r = chunk(i, RC)
            x = jnp.exp2(scores(v, b, r) * (LOG2E / TEMP_TAU))
            e[v, b, r, :] = x
            s = lanes(x)
            dsum[v, n // 2, r, :] = dsum[v, n // 2, r, :] + s if n % 2 else s
            x = x * x
            a2[v, b, r, :] = x
            return acc + subl(x) if n == 0 else acc
        return lax.fori_loop(0, rows // RC, body, jnp.zeros((8, kb), F32))

    own = []
    for v in range(2):
        loads[2 + v].wait()
        own.append(jnp.sum(exp_block(v, p, 0), axis=0, keepdims=True))
    c1b[d * np_ + p] = jnp.concatenate(own, axis=0)
    firsts = []
    for n, (i, j) in enumerate(others):
        me = c1b.at[d * np_ + p]
        cp = remote(me, me, c1send.at[n], c1recv.at[n], (p + i) % np_, (d + j) % nd)
        cp.start()
        firsts.append(cp)

    forwards = []
    for n, b in enumerate(peers):
        got = remote(call.at[b, core], call.at[b, core], csend.at[n], crecv.at[n], b, d)
        got.wait_recv()
        cp = remote(call.at[b, core], call.at[b, core], fsend.at[n], frecv.at[n], p, mate)
        cp.start()
        forwards.append(cp)
    for n, b in enumerate(peers):
        got = remote(call.at[b, 1 - core], call.at[b, 1 - core], fsend.at[n], frecv.at[n], p, mate)
        got.wait_recv()
        for v in range(2):
            exp_block(v, b, n + 1)
    for cp in firsts:
        cp.wait_recv()
    for v in range(2):
        for b in range(np_):
            tot = c1b[b, v:v + 1, :]
            for j in range(1, nd):
                tot = tot + c1b[j * np_ + b, v:v + 1, :]
            vb[v, b] = jnp.broadcast_to(1.0 / (nk * tot), (8, kb))

    def scaled(v, b, r):
        n = r.size // 8
        return (a2[v, b, r, :].reshape(n, 8, kb) * vb[v, b][None]).reshape(n * 8, kb)

    def rowsum(v, r):
        acc = lanes(scaled(v, 0, r))
        for b in range(1, np_):
            acc = acc + lanes(scaled(v, b, r))
        return jnp.sum(acc, axis=1, keepdims=True)

    R2 = 128

    def sweep(v):
        def body(i, accs):
            r = chunk(i, R2)
            u = 1.0 / (nrows * rowsum(v, r))
            return tuple(accs[b] + subl(a2[v, b, r, :] * u) for b in range(np_))
        return lax.fori_loop(0, rows // R2, body, tuple(jnp.zeros((8, kb), F32) for _ in range(np_)))

    def exchange(it, v, accs):
        slot = (it * 2 + v) * nd
        for b in range(np_):
            cb[slot + d, :, b * kb:(b + 1) * kb] = jnp.sum(accs[b], axis=0, keepdims=True)
        out = []
        for q in range(1, nd):
            me = cb.at[slot + d]
            cp = remote(me, me, bsend.at[slot + q], brecv.at[slot + q], p, (d + q) % nd)
            cp.start()
            out.append(cp)
        return out

    def finish(it, v, copies):
        slot = (it * 2 + v) * nd
        for cp in copies:
            cp.wait_recv()
        tot = cb[slot]
        for j in range(1, nd):
            tot = tot + cb[slot + j]
        inv = 1.0 / (nk * tot)
        for b in range(np_):
            vb[v, b] = jnp.broadcast_to(inv[:, b * kb:(b + 1) * kb], (8, kb))

    scale = 1.0 / (2 * nrows * TEMP_TAU)

    def wide(x):
        return jnp.concatenate([x, x], axis=1)

    R3 = 128

    def own_part(v, lacc):
        w = 1 - v

        def body(i, lacc):
            r = chunk(i, R3)
            rinv = jnp.broadcast_to(1.0 / rowsum(v, r), (R3, 128))
            rsc = rinv * scale
            rs[v, r, :] = rsc
            den = jnp.broadcast_to(jnp.sum(dsum[w, 0, r, :] + dsum[w, 1, r, :], axis=1, keepdims=True), (R3, 128))
            dsc = scale / den
            di[w, r, :] = dsc
            t = scaled(v, p, r)
            q = t * wide(rinv)
            codes[v][r, :] = q
            hown[w, r, :] = (e[w, p, r, :] * wide(dsc) - t * wide(rsc)).astype(jnp.bfloat16)
            logp = scores(w, p, r) * (1.0 / TEMP_TAU) - wide(jnp.log(den))
            return lacc + subl(lanes(q * logp))

        return lax.fori_loop(0, rows // R3, body, lacc)

    def dc_part(w):
        return lax.dot_general(hown[w], z[w], (((0,), (0,)), ((), ())), preferred_element_type=F32)

    pend, sends = [None, None], []
    for it in range(ITERS - 1):
        for v in range(2):
            if it:
                finish(it - 1, v, pend[v])
            pend[v] = exchange(it, v, sweep(v))
            sends += pend[v]
    lacc = jnp.zeros((8, 128), F32)
    finish(ITERS - 2, 0, pend[0])
    lacc = own_part(0, lacc)
    finish(ITERS - 2, 1, pend[1])
    lacc = own_part(1, lacc)
    dcp[...] = (dc_part(0) + dc_part(1)).reshape(dcp.shape)

    s1 = remote(dcp.at[1 - core], dcr.at[0], dsend.at[0], drecv.at[0], p, mate)
    s1.start()
    lossb[d * np_ + p] = jnp.broadcast_to(jnp.sum(lacc).reshape(1, 1), (1, 128))
    lcopies = []
    for n, (i, j) in enumerate(others):
        me = lossb.at[d * np_ + p]
        cp = remote(me, me, lsend.at[n], lrecv.at[n], (p + i) % np_, (d + j) % nd)
        cp.start()
        lcopies.append(cp)

    def grad_part(lo, hi):
        def body(i, carry):
            r = chunk(i, R3)
            acc = None
            for b in range(np_):
                hs = [e[w, b, r, :] * wide(di[w, r, :]) - scaled(1 - w, b, r) * wide(rs[1 - w, r, :]) for w in range(2)]
                x = jnp.dot(jnp.concatenate(hs, axis=0).astype(jnp.bfloat16), call[b].reshape(kb, call.shape[3]),
                            preferred_element_type=F32)
                acc = x if acc is None else acc + x
            for w in range(2):
                grads[w][r, :] = acc[w * R3:(w + 1) * R3]
            return carry
        lax.fori_loop(lo, hi, body, 0)

    steps = rows // R3
    cut = steps // 4
    grad_part(0, cut)
    s1.wait_recv()
    dcs[...] = dcp[core] + dcr[0]
    s2 = remote(dcs, dcr.at[1], dsend.at[1], drecv.at[1], p, across)
    s2.start()
    grad_part(cut, steps)
    for cp in lcopies:
        cp.wait_recv()
    tot = lossb[0]
    for n in range(1, np_ * nd):
        tot = tot + lossb[n]
    loss_ref[0, 0] = jnp.sum(tot[:, :1]) * (-1.0 / (2 * nrows))
    s2.wait_recv()
    mine = gc.at[pl.ds(pl.multiple_of(core * half, half), half), :]
    mine[...] = dcs[...] + dcr[1]
    s3 = remote(mine, mine, dsend.at[2], drecv.at[2], p, mate)
    s3.start()
    s3.wait_recv()
    for cp in gathers + firsts + forwards + sends + [s1, s2, s3] + lcopies:
        cp.wait_send()


def write_out(*refs):
    n = (len(refs) - 1) // 2
    copies = [pltpu.make_async_copy(refs[i], refs[n + i], refs[-1].at[i]) for i in range(n)]
    for cp in copies:
        cp.start()
    for cp in copies:
        cp.wait()


def solution(mesh):
    np_, nd = mesh.shape["proto"], mesh.shape["data"]

    def step(emb_one, emb_two, protos):
        rows, dim = emb_one.shape
        kb = protos.shape[0]
        n, dma = np_ * nd, pltpu.SemaphoreType.DMA
        nx = (ITERS - 1) * 2 * nd
        vm, hbm = pl.BlockSpec(memory_space=pltpu.VMEM), pl.BlockSpec(memory_space=pltpu.HBM)
        sds = jax.ShapeDtypeStruct
        code1, code2, loss, g1, g2, gc = pl.pallas_call(
            functools.partial(kernel, np_, nd),
            out_shape=(pltpu.VMEM((rows, kb), F32), pltpu.VMEM((rows, kb), F32), sds((1, 1), F32),
                       pltpu.VMEM((rows, dim), F32), pltpu.VMEM((rows, dim), F32), pltpu.VMEM((kb, dim), F32)),
            in_specs=[hbm] * 3,
            out_specs=(vm, vm, pl.BlockSpec(memory_space=pltpu.SMEM), vm, vm, vm),
            scratch_shapes=[
                pltpu.VMEM((2, rows, dim), jnp.bfloat16),
                pltpu.VMEM((np_, 2, kb // 2, dim), jnp.bfloat16),
                pltpu.VMEM((2, np_, rows, kb), F32),
                pltpu.VMEM((2, np_, rows, kb), F32),
                pltpu.VMEM((n, 2, kb), F32),
                pltpu.VMEM((nx, 1, np_ * kb), F32),
                pltpu.VMEM((2, 2, rows, 128), F32),
                pltpu.VMEM((2, rows, 128), F32),
                pltpu.VMEM((2, rows, 128), F32),
                pltpu.VMEM((2, rows, kb), jnp.bfloat16),
                pltpu.VMEM((2, np_, 8, kb), F32),
                pltpu.VMEM((2, kb // 2, dim), F32),
                pltpu.VMEM((2, kb // 2, dim), F32),
                pltpu.VMEM((kb // 2, dim), F32),
                pltpu.VMEM((n, 1, 128), F32),
                dma((4,)), dma((3,)), dma((3,)), dma((3,)), dma((3,)), dma((n - 1,)), dma((n - 1,)),
                dma((nx,)), dma((nx,)), dma((3,)), dma((3,)), dma((n - 1,)), dma((n - 1,)),
            ],
            compiler_params=pltpu.CompilerParams(collective_id=0, has_side_effects=True,
                                                 vmem_limit_bytes=VMEM_MIB * 1024 * 1024),
        )(*(pltpu.with_memory_space_constraint(x, pltpu.HBM) for x in (emb_one, emb_two, protos)))
        big = (code1, code2, g1, g2, gc)
        code1, code2, g1, g2, gc = pl.pallas_call(
            write_out,
            out_shape=tuple(sds(x.shape, F32) for x in big),
            in_specs=[vm] * len(big),
            out_specs=(hbm,) * len(big),
            scratch_shapes=[dma((len(big),))],
            compiler_params=pltpu.CompilerParams(vmem_limit_bytes=1024 * 1024),
        )(*big)
        return code1, code2, loss.reshape(()), g1, g2, gc

    return jax.shard_map(
        step, mesh=mesh,
        in_specs=(P("data", None), P("data", None), P("proto", None)),
        out_specs=(P("data", "proto"), P("data", "proto"), P(), P("data", None), P("data", None), P("proto", None)),
        check_vma=False)
```

```python
import functools
import math

import jax
import jax.numpy as jnp
from jax import lax
from jax.experimental import pallas as pl
from jax.experimental.pallas import tpu as pltpu
from jax.sharding import PartitionSpec as P

EPSILON = 0.05
TEMP_TAU = 0.1
ITERS = 3
VMEM_MIB = 40
MESH = pl.DeviceIdType.MESH
F32 = jnp.float32
LOG2E = math.log2(math.e)


def lanes(x):
    total = x[:, :128]
    for i in range(1, x.shape[1] // 128):
        total = total + x[:, i * 128:(i + 1) * 128]
    return total


def subl(x):
    return jnp.sum(x.reshape(x.shape[0] // 8, 8, x.shape[1]), axis=0)


def kernel(np_, nd, z1_ref, z2_ref, c_ref,
           code1, code2, loss_ref, g1, g2, gc,
           z, call, a2, c1b, c1t, cb, dsum, di, rs, hown, vb, dcp, dcr, dcs, lossb, losst,
           lsem, csend, crecv, fsend, frecv, bsend, brecv, dsend, drecv, tsend, trecv):
    rows, kb = z.shape[1], 2 * call.shape[2]
    nrows, nk = rows * nd, kb * np_
    p, d = lax.axis_index("proto"), lax.axis_index("data")
    core = d % 2
    mate, across = d + 1 - 2 * core, (d + 2) % nd
    codes, grads = (code1, code2), (g1, g2)
    near = p + 1 - 2 * (p % 2)
    peers = (near, (p + 2) % np_, (near + 2) % np_)

    def remote(src, dst, ss, rsem, pp, dd):
        return pltpu.make_async_remote_copy(src_ref=src, dst_ref=dst, send_sem=ss, recv_sem=rsem,
                                            device_id={"proto": pp, "data": dd}, device_id_type=MESH)

    half = kb // 2
    loads = [pltpu.make_async_copy(c_ref.at[pl.ds(0, half), :], call.at[p, 0], lsem.at[0]),
             pltpu.make_async_copy(c_ref.at[pl.ds(half, half), :], call.at[p, 1], lsem.at[1]),
             pltpu.make_async_copy(z1_ref, z.at[0], lsem.at[2]),
             pltpu.make_async_copy(z2_ref, z.at[1], lsem.at[3])]
    for cp in loads:
        cp.start()
    ring = [(d + j) % nd for j in range(1, nd)]
    barrier = pltpu.get_barrier_semaphore()
    for pp, dd in [(b, d) for b in peers] + [(p, j) for j in ring]:
        pl.semaphore_signal(barrier, inc=1, device_id={"proto": pp, "data": dd}, device_id_type=MESH)
    loads[0].wait()
    loads[1].wait()
    pl.semaphore_wait(barrier, np_ + nd - 2)

    gathers = []
    for n, peer in enumerate(peers):
        cp = remote(call.at[p, core], call.at[p, core], csend.at[n], crecv.at[n], peer, d)
        cp.start()
        gathers.append(cp)

    def scores(v, b, r):
        return lax.dot_general(z[v, r, :], call[b].reshape(kb, call.shape[3]), (((1,), (1,)), ((), ())),
                               preferred_element_type=F32)

    def chunk(i, size):
        return pl.ds(pl.multiple_of(i * size, size), size)

    def to_data(me, slot):
        out = []
        for q, dd in enumerate(ring):
            cp = remote(me, me, bsend.at[slot + q], brecv.at[slot + q], p, dd)
            cp.start()
            out.append(cp)
        return out

    def to_proto(me, k):
        out = []
        for n, b in enumerate(peers):
            cp = remote(me, me, tsend.at[k + n], trecv.at[k + n], b, d)
            cp.start()
            out.append(cp)
        return out

    def arrived(copies):
        for cp in copies:
            cp.wait_recv()

    RC = 256

    def exp_block(v, b, n):
        def body(i, acc):
            for r in (chunk(2 * i, RC), chunk(2 * i + 1, RC)):
                x = jnp.exp2(scores(v, b, r) * (LOG2E / TEMP_TAU))
                t = lanes(x)
                dsum[v, n // 2, r, :] = dsum[v, n // 2, r, :] + t if n % 2 else t
                x = x * x
                a2[v, b, r, :] = x
                if n == 0:
                    acc = acc + subl(x)
            return acc
        return lax.fori_loop(0, rows // RC // 2, body, jnp.zeros((8, kb), F32))

    own = []
    for v in range(2):
        loads[2 + v].wait()
        own.append(jnp.sum(exp_block(v, p, 0), axis=0, keepdims=True))
    c1b[d] = jnp.concatenate(own, axis=0)
    firsts = to_data(c1b.at[d], 0)

    forwards = []

    def forward(n):
        b = peers[n]
        remote(call.at[b, core], call.at[b, core], csend.at[n], crecv.at[n], b, d).wait_recv()
        cp = remote(call.at[b, core], call.at[b, core], fsend.at[n], frecv.at[n], p, mate)
        cp.start()
        forwards.append(cp)

    def use(n):
        b = peers[n]
        remote(call.at[b, 1 - core], call.at[b, 1 - core], fsend.at[n], frecv.at[n], p, mate).wait_recv()
        for v in range(2):
            exp_block(v, b, n + 1)

    def total(ref, n):
        tot = ref[0]
        for j in range(1, n):
            tot = tot + ref[j]
        return tot

    forward(0)
    forward(1)
    arrived(firsts)
    c1t[p] = total(c1b, nd)
    seconds = to_proto(c1t.at[p], 0)
    use(0)
    forward(2)
    use(1)
    use(2)
    arrived(seconds)
    for v in range(2):
        for b in range(np_):
            vb[v, b] = jnp.broadcast_to(1.0 / (nk * c1t[b, v:v + 1, :]), (8, kb))

    def scaled(v, b, r):
        n = r.size // 8
        return (a2[v, b, r, :].reshape(n, 8, kb) * vb[v, b][None]).reshape(n * 8, kb)

    def rowsum(v, r):
        acc = lanes(scaled(v, 0, r))
        for b in range(1, np_):
            acc = acc + lanes(scaled(v, b, r))
        return jnp.sum(acc, axis=1, keepdims=True)

    R2 = 128

    def sweep(v):
        def body(i, accs):
            r = chunk(i, R2)
            u = 1.0 / (nrows * rowsum(v, r))
            return tuple(accs[b] + subl(a2[v, b, r, :] * u) for b in range(np_))
        return lax.fori_loop(0, rows // R2, body, tuple(jnp.zeros((8, kb), F32) for _ in range(np_)))

    def exchange(it, v, accs):
        slot = it * 2 + v
        for b in range(np_):
            cb[slot * nd + d, :, b * kb:(b + 1) * kb] = jnp.sum(accs[b], axis=0, keepdims=True)
        return to_data(cb.at[slot * nd + d], (slot + 1) * (nd - 1))

    def finish(it, v, copies):
        arrived(copies)
        tot = cb[(it * 2 + v) * nd]
        for j in range(1, nd):
            tot = tot + cb[(it * 2 + v) * nd + j]
        inv = 1.0 / (nk * tot)
        for b in range(np_):
            vb[v, b] = jnp.broadcast_to(inv[:, b * kb:(b + 1) * kb], (8, kb))

    scale = 1.0 / (2 * nrows * TEMP_TAU)

    def wide(x):
        return jnp.concatenate([x, x], axis=1)

    R3 = 128

    def dens():
        def body(i, carry):
            r = chunk(i, R3)
            for v in range(2):
                den = jnp.sum(dsum[v, 0, r, :] + dsum[v, 1, r, :], axis=1, keepdims=True)
                di[v, r, :] = jnp.broadcast_to(scale / den, (R3, 128))
                dsum[v, 0, r, :] = jnp.broadcast_to(jnp.log(den), (R3, 128))
            return carry
        lax.fori_loop(0, rows // R3, body, 0)

    R4 = 256

    def own_part(v, lacc):
        w = 1 - v

        def body(i, lacc):
            r = chunk(i, R4)
            rinv = jnp.broadcast_to(1.0 / rowsum(v, r), (R4, 128))
            rsc = rinv * scale
            rs[v, r, :] = rsc
            t = scaled(v, p, r)
            q = t * wide(rinv)
            codes[v][r, :] = q
            x = a2[w, p, r, :]
            hw = (x * lax.rsqrt(x) * wide(di[w, r, :]) - t * wide(rsc)).astype(jnp.bfloat16)
            hown[w, 0, r, :] = hw[:, :half]
            hown[w, 1, r, :] = hw[:, half:]
            logp = scores(w, p, r) * (1.0 / TEMP_TAU) - wide(dsum[w, 0, r, :])
            return lacc + subl(lanes(q * logp))

        return lax.fori_loop(0, rows // R4, body, lacc)

    def dc_part(w, k):
        return lax.dot_general(hown[w, k], z[w], (((0,), (0,)), ((), ())), preferred_element_type=F32)

    pend, sends = [None, None], []
    for it in range(ITERS - 1):
        for v in range(2):
            if it:
                finish(it - 1, v, pend[v])
            pend[v] = exchange(it, v, sweep(v))
            sends += pend[v]
        if it == 0:
            dens()
    lacc = jnp.zeros((8, 128), F32)
    finish(ITERS - 2, 0, pend[0])
    lacc = own_part(0, lacc)
    finish(ITERS - 2, 1, pend[1])
    lacc = own_part(1, lacc)
    dcp[0] = dc_part(0, 1 - core) + dc_part(1, 1 - core)
    s1 = remote(dcp.at[0], dcr.at[0], dsend.at[0], drecv.at[0], p, mate)
    s1.start()
    lossb[d] = jnp.broadcast_to(jnp.sum(lacc).reshape(1, 1), (1, 128))
    lcopies = to_data(lossb.at[d], (2 * ITERS - 1) * (nd - 1))
    dcp[1] = dc_part(0, core) + dc_part(1, core)

    def root(v, b, r):
        x = a2[v, b, r, :]
        return x * lax.rsqrt(x)

    def grad_part(lo, hi):
        def body(i, carry):
            r = chunk(i, R3)
            acc = None
            for b in range(np_):
                hs = [root(w, b, r) * wide(di[w, r, :]) - scaled(1 - w, b, r) * wide(rs[1 - w, r, :]) for w in range(2)]
                x = jnp.dot(jnp.concatenate(hs, axis=0).astype(jnp.bfloat16), call[b].reshape(kb, call.shape[3]),
                            preferred_element_type=F32)
                acc = x if acc is None else acc + x
            for w in range(2):
                grads[w][r, :] = acc[w * R3:(w + 1) * R3]
            return carry
        lax.fori_loop(lo, hi, body, 0)

    steps = rows // R3
    cut = steps // 4
    grad_part(0, cut)
    s1.wait_recv()
    dcs[...] = dcp[1] + dcr[0]
    s2 = remote(dcs, dcr.at[1], dsend.at[1], drecv.at[1], p, across)
    s2.start()
    arrived(lcopies)
    losst[p] = total(lossb, nd)
    lfinal = to_proto(losst.at[p], np_ - 1)
    grad_part(cut, steps)
    arrived(lfinal)
    loss_ref[0, 0] = jnp.sum(total(losst, np_)[:, :1]) * (-1.0 / (2 * nrows))
    s2.wait_recv()
    mine = gc.at[pl.ds(pl.multiple_of(core * half, half), half), :]
    mine[...] = dcs[...] + dcr[1]
    s3 = remote(mine, mine, dsend.at[2], drecv.at[2], p, mate)
    s3.start()
    s3.wait_recv()
    for cp in gathers + firsts + seconds + forwards + sends + [s1, s2, s3] + lcopies + lfinal:
        cp.wait_send()


def write_out(*refs):
    n = (len(refs) - 1) // 2
    copies = [pltpu.make_async_copy(refs[i], refs[n + i], refs[-1].at[i]) for i in range(n)]
    for cp in copies:
        cp.start()
    for cp in copies:
        cp.wait()


def solution(mesh):
    np_, nd = mesh.shape["proto"], mesh.shape["data"]

    def step(emb_one, emb_two, protos):
        rows, dim = emb_one.shape
        kb = protos.shape[0]
        dma = pltpu.SemaphoreType.DMA
        nx, nsem = (ITERS - 1) * 2 * nd, 2 * ITERS * (nd - 1)
        vm, hbm = pl.BlockSpec(memory_space=pltpu.VMEM), pl.BlockSpec(memory_space=pltpu.HBM)
        sds = jax.ShapeDtypeStruct
        code1, code2, loss, g1, g2, gc = pl.pallas_call(
            functools.partial(kernel, np_, nd),
            out_shape=(pltpu.VMEM((rows, kb), F32), pltpu.VMEM((rows, kb), F32), sds((1, 1), F32),
                       pltpu.VMEM((rows, dim), F32), pltpu.VMEM((rows, dim), F32), pltpu.VMEM((kb, dim), F32)),
            in_specs=[hbm] * 3,
            out_specs=(vm, vm, pl.BlockSpec(memory_space=pltpu.SMEM), vm, vm, vm),
            scratch_shapes=[
                pltpu.VMEM((2, rows, dim), jnp.bfloat16),
                pltpu.VMEM((np_, 2, kb // 2, dim), jnp.bfloat16),
                pltpu.VMEM((2, np_, rows, kb), F32),
                pltpu.VMEM((nd, 2, kb), F32),
                pltpu.VMEM((np_, 2, kb), F32),
                pltpu.VMEM((nx, 1, np_ * kb), F32),
                pltpu.VMEM((2, 2, rows, 128), F32),
                pltpu.VMEM((2, rows, 128), F32),
                pltpu.VMEM((2, rows, 128), F32),
                pltpu.VMEM((2, 2, rows, kb // 2), jnp.bfloat16),
                pltpu.VMEM((2, np_, 8, kb), F32),
                pltpu.VMEM((2, kb // 2, dim), F32),
                pltpu.VMEM((2, kb // 2, dim), F32),
                pltpu.VMEM((kb // 2, dim), F32),
                pltpu.VMEM((nd, 1, 128), F32),
                pltpu.VMEM((np_, 1, 128), F32),
                dma((4,)), dma((np_ - 1,)), dma((np_ - 1,)), dma((np_ - 1,)), dma((np_ - 1,)),
                dma((nsem,)), dma((nsem,)), dma((3,)), dma((3,)), dma((2 * np_ - 2,)), dma((2 * np_ - 2,)),
            ],
            compiler_params=pltpu.CompilerParams(collective_id=0, has_side_effects=True,
                                                 vmem_limit_bytes=VMEM_MIB * 1024 * 1024),
        )(*(pltpu.with_memory_space_constraint(x, pltpu.HBM) for x in (emb_one, emb_two, protos)))
        big = (code1, code2, g1, g2, gc)
        code1, code2, g1, g2, gc = pl.pallas_call(
            write_out,
            out_shape=tuple(sds(x.shape, F32) for x in big),
            in_specs=[vm] * len(big),
            out_specs=(hbm,) * len(big),
            scratch_shapes=[dma((len(big),))],
            compiler_params=pltpu.CompilerParams(vmem_limit_bytes=1024 * 1024),
        )(*big)
        return code1, code2, loss.reshape(()), g1, g2, gc

    return jax.shard_map(
        step, mesh=mesh,
        in_specs=(P("data", None), P("data", None), P("proto", None)),
        out_specs=(P("data", "proto"), P("data", "proto"), P(), P("data", None), P("data", None), P("proto", None)),
        check_vma=False)
```
